32 devices in a mesh: reps: 2 (over x), grow: 16 (over z, y, core).
Axes of the slice: x: 2, y: 2, z: 4, core: 2. Of those that a mesh axis runs over, the one named last changes fastest.
Arguments:
- hamiltonian: float32 [192, 3, 256, 256], P(('reps', 'grow')), parts along dimension 0, may hold values from -3 to 3, as said below
- pattern: int32 [96, 3], replicated, may hold values from 0 to 1, as said below
- potential: float32 [2], P('reps'), parts along dimension 0, may hold values from -0.2 to 0.2
Outputs:
- sign_matrix: float32 [192, 3, 256, 256], P(('reps', 'grow')), parts along dimension 0
- occupation: float32 [2], P('reps'), parts along dimension 0
The draws below stay inside these ranges and needn't reach their ends.
There are 2 independent parts, one for each index of `reps`. The reference program is written for one: setup_inputs(seed, part) draws one part's arguments, and reference() takes and returns one part's arrays. A program takes and returns all parts, laid end to end along the dimension named above; an argument that names none is the same for every part. Nothing has to cross between parts.
Inputs may be any that keep to these rules, and one draw needn't show every extreme that they name: `hamiltonian`: the matrix is symmetric: slot 2 of block row i is the transpose of slot 0 of block row i + 1, slot 1 is symmetric, slot 0 of row 0 and slot 2 of row 95 are zero. pattern[i, 1] = 1; pattern[i, 2] = pattern[i + 1, 0]; pattern[0, 0] = pattern[95, 2] = 0.
All inputs are finite; a program needn't handle non-finite values.
Results may differ from the reference program's by a relative error of at most 0.0001.
Values sent between devices are 32-bit elements; how exact they have to be, the bound alone decides.
A program may use at most 64 MiB of HBM per device.

```python
import math
import jax
import jax.numpy as jnp
from jax import lax

BS = 256
ROWS_DEV = 6
ITERS = 2
NBLK = 96


def draw_hamiltonian(key, part):
    key_diag, key_rough, key_upper = jax.random.split(key, 3)
    spread = 0.25 / math.sqrt(3.0 * BS)
    levels = jnp.arange(NBLK, dtype=jnp.float32)
    centre = 0.5 - levels / max(NBLK - 1, 1)
    inner_raw = jax.random.normal(key_diag, (NBLK, BS, BS), jnp.float32) * spread
    upper_raw = jax.random.normal(key_upper, (NBLK, BS, BS), jnp.float32) * spread
    roughness = jax.random.uniform(key_rough, (NBLK, BS), jnp.float32, -0.3, 0.3)
    unit_block = jnp.eye(BS, dtype=jnp.float32)
    diagonal = (inner_raw + jnp.swapaxes(inner_raw, 1, 2)) * 0.7071 + (centre[:, None] + roughness)[:, :, None] * unit_block[None]
    zero_block = jnp.zeros((1, BS, BS), jnp.float32)
    below_block = jnp.concatenate([zero_block, jnp.swapaxes(upper_raw[:-1], 1, 2)], axis=0)
    above_block = jnp.concatenate([upper_raw[:-1], zero_block], axis=0)
    return jnp.stack([below_block, diagonal, above_block], axis=1)


def draw_pattern(key, part):
    choose = jax.random.randint(key, (NBLK - 1,), 0, 5)
    lower_row = jnp.arange(1, NBLK, dtype=jnp.int32)
    boundary = (lower_row % ROWS_DEV == 0).astype(jnp.int32)
    edge_kept = jnp.maximum((choose < 3).astype(jnp.int32), boundary)
    nothing = jnp.zeros((1,), jnp.int32)
    return jnp.stack([jnp.concatenate([nothing, edge_kept]), jnp.ones((NBLK,), jnp.int32), jnp.concatenate([edge_kept, nothing])], axis=1)


def setup_inputs(seed: int = 0, part: int = 0) -> dict:
    seeds = jax.random.split(jax.random.key(seed), 4)
    part_splits = jax.random.split(jax.random.fold_in(seeds[3], part), 4)
    hamiltonian = draw_hamiltonian(jax.random.fold_in(jax.random.fold_in(seeds[3], part), 71), part)
    pattern = draw_pattern(jax.random.fold_in(seeds[3], 71), part)
    potential = jnp.clip(jax.random.uniform(part_splits[2], (1,), jnp.float32, -0.2, 0.2), -0.2, 0.2)
    return dict(hamiltonian=hamiltonian, pattern=pattern, potential=potential)


def banded(operand, extended, keep_mask):
    row_count = operand.shape[0]
    columns = []
    for column in range(3):
        summed = jnp.zeros_like(operand[:, 0])
        for source in range(3):
            partner = column - source + 1
            if 0 <= partner < 3:
                summed = summed + jnp.einsum("rij,rjk->rik", operand[:, source], extended[source:source + row_count, partner], precision=lax.Precision.HIGHEST)
        columns.append(summed)
    return jnp.stack(columns, axis=1) * keep_mask[:, :, None, None]


def padded_rows(field):
    return jnp.pad(field, ((1, 1), (0, 0), (0, 0), (0, 0)))


def reference(hamiltonian, pattern, potential):
    keep_mask = pattern.astype(jnp.float32)
    unit_block = jnp.eye(BS, dtype=jnp.float32)
    slot_weight = (jnp.arange(3) == 1).astype(jnp.float32)
    identity_band = slot_weight[None, :, None, None] * unit_block[None, None]
    current = (potential[0] * identity_band - hamiltonian) * keep_mask[:, :, None, None]
    for iteration in range(ITERS):
        square = banded(current, padded_rows(current), keep_mask)
        shifted = (3.0 * identity_band - square) * keep_mask[:, :, None, None]
        current = 0.5 * banded(current, padded_rows(shifted), keep_mask)
    total_trace = jnp.sum(jnp.trace(current[:, 1], axis1=1, axis2=2))
    matrix_order = float(NBLK * BS)
    occupation = ((matrix_order + total_trace) / (2.0 * matrix_order)).reshape(1)
    return current, occupation
```

```python
import functools

import jax
import jax.numpy as jnp
from jax import lax
from jax.experimental import pallas as pl
from jax.experimental.pallas import tpu as pltpu
from jax.sharding import PartitionSpec as P

F32 = jnp.float32
BF16 = jnp.bfloat16
PIECES = 4
MESH = pl.DeviceIdType.MESH


def product(left, right, left_at, right_at, transposed=False):
    (lh, ll), (rh, rl) = left, right
    dims = (((1,), (1 if transposed else 0,)), ((), ()))

    def dot(a, b):
        return lax.dot_general(a, b, dims, preferred_element_type=F32)

    a_hi, a_lo, b_hi, b_lo = lh[left_at], ll[left_at], rh[right_at], rl[right_at]
    return (dot(a_lo, b_hi) + dot(a_hi, b_lo)) + dot(a_hi, b_hi)


def store(pair, at, value):
    high = value.astype(BF16)
    pair[0][at] = high
    pair[1][at] = (value - high.astype(F32)).astype(BF16)


def kernel(n, h, pattern, potential, out, occupation, *scratch):
    (stage, result, before, after, parts, trace_tile, ah, al, sh, sl, crh, crl, cch, ccl, s2h, s2l,
     load_sem, store_sem, next_send, next_recv, prev_send, prev_recv, part_send, part_recv) = scratch
    rows, edge = h.shape[0], h.shape[2]
    row_total = pattern.shape[0]
    me = lax.axis_index("grow")
    has_prev, has_next = me > 0, me < n - 1
    a, s, cr, cc, s2 = (ah, al), (sh, sl), (crh, crl), (cch, ccl), (s2h, s2l)

    loads = [pltpu.make_async_copy(h.at[r], stage.at[r], load_sem.at[r]) for r in range(rows)]
    for load in loads:
        load.start()

    barrier = pltpu.get_barrier_semaphore()

    @pl.loop(1, n)
    def _(k):
        pl.semaphore_signal(barrier, inc=1, device_id={"grow": lax.rem(me + k, n)}, device_id_type=MESH)

    pl.semaphore_wait(barrier, n - 1)

    last = rows - 1
    to_next = [
        pltpu.make_async_remote_copy(
            src_ref=h.at[r, c], dst_ref=before.at[p], send_sem=next_send.at[p], recv_sem=next_recv.at[p],
            device_id={"grow": lax.rem(me + 1, n)}, device_id_type=MESH)
        for p, (r, c) in enumerate([(last, 1), (last, 0), (last - 1, 1), (last - 1, 0)])
    ]
    to_prev = [
        pltpu.make_async_remote_copy(
            src_ref=h.at[r, c], dst_ref=after.at[p], send_sem=prev_send.at[p], recv_sem=prev_recv.at[p],
            device_id={"grow": lax.rem(me + n - 1, n)}, device_id_type=MESH)
        for p, (r, c) in enumerate([(0, 1), (0, 2), (1, 1), (1, 2)])
    ]

    @pl.when(has_next)
    def _():
        for copy in to_next:
            copy.start()

    @pl.when(has_prev)
    def _():
        for copy in to_prev:
            copy.start()

    @pl.when(jnp.logical_not(has_prev))
    def _():
        before[...] = jnp.zeros_like(before)

    @pl.when(jnp.logical_not(has_next))
    def _():
        after[...] = jnp.zeros_like(after)

    def arrive(p):
        @pl.when(has_prev)
        def _():
            to_next[p].wait_recv()

        @pl.when(has_next)
        def _():
            to_prev[p].wait_recv()

    def on_diagonal():
        return lax.broadcasted_iota(jnp.int32, (edge, edge), 0) == lax.broadcasted_iota(
            jnp.int32, (edge, edge), 1)

    def mask(e, c):
        row = jnp.clip(me * rows + e - 2, 0, row_total - 1)
        return pattern[row, c].astype(F32)

    def lanes(c):
        return slice(c * edge, (c + 1) * edge)

    def put_a(e, c, block):
        value = -block
        if c == 1:
            value = jnp.where(on_diagonal(), potential[0] + value, value)
        store(a, (e, slice(None), lanes(c)), value * mask(e, c))

    left_of = {0: slice(0, 2 * edge), 1: slice(0, 3 * edge), 2: slice(edge, 3 * edge)}
    right_of = {0: slice(edge, 3 * edge), 1: slice(0, 3 * edge), 2: slice(0, 2 * edge)}
    full = slice(None)

    def filtered(left, right, e, c, transposed=False):
        right_at = (e + c - 1, full, right_of[c]) if transposed else (e + c - 1, right_of[c], full)
        return product(left, right, (e, full, left_of[c]), right_at, transposed)

    def shifted(square, e, c):
        value = -square
        if c == 1:
            value = jnp.where(on_diagonal(), 3.0 + value, value)
        return value * mask(e, c)

    def column_at(e, c):
        return (e + c - 1, lanes(2 - c), full)

    def f1(e, slots=(0, 1, 2)):
        for c in slots:
            store(s, column_at(e, c), shifted(filtered(a, a, e, c, True), e, c))

    def f2(e, slots=(0, 1, 2)):
        for c in slots:
            value = filtered(a, s, e, c) * (0.5 * mask(e, c))
            store(cr, (e, full, lanes(c)), value)
            store(cc, column_at(e, c), value)

    def f3(e, slots=(0, 1, 2)):
        for c in slots:
            store(s2, column_at(e, c), shifted(filtered(cr, cc, e, c), e, c))

    def f4(e):
        for c in range(3):
            value = filtered(cr, s2, e, c) * (0.5 * mask(e, c))
            result[e - 2, c] = value
            if c == 1:
                trace_tile[...] += jnp.sum(jnp.where(on_diagonal(), value, 0.0), axis=0, keepdims=True)
        pltpu.make_async_copy(result.at[e - 2], out.at[e - 2], store_sem.at[e - 2]).start()

    def span(function, low, high):
        pl.loop(low, high)(function)

    def both(function, low, high):
        @pl.loop(0, 2)
        def _(k):
            function(low + k * (high - low))

    trace_tile[...] = jnp.zeros_like(trace_tile)
    lo, hi = 2, rows + 1
    for r in range(rows):
        loads[r].wait()
        for c in range(3):
            put_a(r + 2, c, stage[r, c])
    span(f1, lo + 1, hi)
    span(f2, lo + 2, hi - 1)

    put_a(lo - 1, 2, stage[0, 0].T)
    put_a(hi + 1, 0, stage[last, 2].T)
    arrive(0)
    put_a(lo - 1, 1, before[0])
    put_a(hi + 1, 1, after[0])
    both(f1, lo, hi)
    both(f2, lo + 1, hi - 1)
    span(f3, lo + 2, hi - 1)

    arrive(1)
    put_a(lo - 1, 0, before[1])
    put_a(lo - 2, 2, before[1].T)
    put_a(hi + 1, 2, after[1])
    put_a(hi + 2, 0, after[1].T)
    f1(lo - 1, (1, 2))
    f1(hi + 1, (0, 1))
    both(f2, lo, hi)
    both(f3, lo + 1, hi - 1)
    span(f4, lo + 2, hi - 1)

    arrive(2)
    put_a(lo - 2, 1, before[2])
    put_a(hi + 2, 1, after[2])
    f1(lo - 1, (0,))
    f1(lo - 2, (2,))
    f1(hi + 1, (2,))
    f1(hi + 2, (0,))
    f2(lo - 1, (1, 2))
    f2(hi + 1, (0, 1))
    both(f3, lo, hi)
    f3(lo - 1, (2,))
    f3(hi + 1, (0,))
    both(f4, lo + 1, hi - 1)

    arrive(3)
    put_a(lo - 2, 0, before[3])
    put_a(hi + 2, 2, after[3])
    f1(lo - 2, (1,))
    f1(hi + 2, (1,))
    f2(lo - 1, (0,))
    f2(lo - 2, (2,))
    f2(hi + 1, (2,))
    f2(hi + 2, (0,))
    f3(lo - 1, (1,))
    f3(hi + 1, (1,))
    both(f4, lo, hi)

    parts[me] = jnp.broadcast_to(trace_tile[...], parts.shape[1:])

    def part_copy(target, slot):
        return pltpu.make_async_remote_copy(
            src_ref=parts.at[me], dst_ref=parts.at[me], send_sem=part_send.at[target],
            recv_sem=part_recv.at[slot], device_id={"grow": target}, device_id_type=MESH)

    @pl.loop(1, n)
    def _(k):
        part_copy(lax.rem(me + k, n), me).start()

    for r in range(rows):
        pltpu.make_async_copy(result.at[r], out.at[r], store_sem.at[r]).wait()

    @pl.when(has_next)
    def _():
        for copy in to_next:
            copy.wait_send()

    @pl.when(has_prev)
    def _():
        for copy in to_prev:
            copy.wait_send()

    @pl.loop(1, n)
    def _(k):
        other = lax.rem(me + k, n)
        copy = part_copy(other, other)
        copy.wait_recv()
        copy.wait_send()

    order = float(row_total * edge)
    total = jnp.sum(jnp.sum(parts[...], axis=0)[0:1])
    occupation[0] = (order + total) / (2.0 * order)


def local(n, hamiltonian, pattern, potential):
    rows, edge = hamiltonian.shape[0], hamiltonian.shape[2]
    wide, tall = (rows + 4, edge, 3 * edge), (rows + 4, 3 * edge, edge)
    pairs = [wide, tall, wide, tall, tall]
    any_space = pl.BlockSpec(memory_space=pl.ANY)
    scalars = pl.BlockSpec(memory_space=pltpu.SMEM)
    sems = pltpu.SemaphoreType.DMA
    return pl.pallas_call(
        functools.partial(kernel, n),
        out_shape=(jax.ShapeDtypeStruct(hamiltonian.shape, F32), jax.ShapeDtypeStruct((1,), F32)),
        in_specs=[any_space, scalars, scalars],
        out_specs=(any_space, scalars),
        scratch_shapes=[
            pltpu.VMEM((rows, 3, edge, edge), F32),
            pltpu.VMEM((rows, 3, edge, edge), F32),
            pltpu.VMEM((PIECES, edge, edge), F32),
            pltpu.VMEM((PIECES, edge, edge), F32),
            pltpu.VMEM((n, 8, edge), F32),
            pltpu.VMEM((1, edge), F32),
            *[pltpu.VMEM(shape, BF16) for shape in pairs for _ in range(2)],
            sems((rows,)), sems((rows,)), sems((PIECES,)), sems((PIECES,)), sems((PIECES,)), sems((PIECES,)),
            sems((n,)), sems((n,)),
        ],
        compiler_params=pltpu.CompilerParams(
            collective_id=0, has_side_effects=True, vmem_limit_bytes=62 * 1024 * 1024),
        name="sign_iterations",
    )(hamiltonian, pattern, potential)


def solution(mesh):
    in_specs = (P(("reps", "grow"), None, None, None), P(), P("reps"))
    out_specs = (P(("reps", "grow"), None, None, None), P("reps"))
    return jax.shard_map(
        functools.partial(local, mesh.shape["grow"]),
        mesh=mesh, in_specs=in_specs, out_specs=out_specs, check_vma=False)
```

```python
import functools

import jax
import jax.numpy as jnp
from jax import lax
from jax.experimental import pallas as pl
from jax.experimental.pallas import tpu as pltpu
from jax.sharding import PartitionSpec as P

F32 = jnp.float32
BF16 = jnp.bfloat16
PIECES = 4
VMEM_LIMIT = 50 * 1024 * 1024
MESH = pl.DeviceIdType.MESH


def product(left, right, left_at, right_at, transposed=False):
    (lh, ll), (rh, rl) = left, right
    dims = (((1,), (1 if transposed else 0,)), ((), ()))

    def dot(a, b):
        return lax.dot_general(a, b, dims, preferred_element_type=F32)

    a_hi, a_lo, b_hi, b_lo = lh[left_at], ll[left_at], rh[right_at], rl[right_at]
    return (dot(a_lo, b_hi) + dot(a_hi, b_lo)) + dot(a_hi, b_hi)


def store(pair, at, value):
    high = value.astype(BF16)
    pair[0][at] = high
    pair[1][at] = (value - high.astype(F32)).astype(BF16)


def kernel(n, h, pattern, potential, out, occupation, *scratch):
    (stage, before, after, parts, trace_tile, ah, al, sh, sl, crh, crl, cch, ccl, s2h, s2l,
     load_sem, next_send, next_recv, prev_send, prev_recv, part_send, part_recv) = scratch
    rows, edge = h.shape[0], h.shape[2]
    row_total = pattern.shape[1]
    me = lax.axis_index("grow")
    has_prev, has_next = me > 0, me < n - 1
    a, s, cr, cc, s2 = (ah, al), (sh, sl), (crh, crl), (cch, ccl), (s2h, s2l)

    loads = [pltpu.make_async_copy(h.at[r], stage.at[r], load_sem.at[r]) for r in range(rows)]
    for load in loads:
        load.start()

    barrier = pltpu.get_barrier_semaphore()

    @pl.loop(1, n)
    def _(k):
        pl.semaphore_signal(barrier, inc=1, device_id={"grow": lax.rem(me + k, n)}, device_id_type=MESH)

    pl.semaphore_wait(barrier, n - 1)

    last = rows - 1
    to_next = [
        pltpu.make_async_remote_copy(
            src_ref=h.at[r, c], dst_ref=before.at[p], send_sem=next_send.at[p], recv_sem=next_recv.at[p],
            device_id={"grow": lax.rem(me + 1, n)}, device_id_type=MESH)
        for p, (r, c) in enumerate([(last, 1), (last, 0), (last - 1, 1), (last - 1, 0)])
    ]
    to_prev = [
        pltpu.make_async_remote_copy(
            src_ref=h.at[r, c], dst_ref=after.at[p], send_sem=prev_send.at[p], recv_sem=prev_recv.at[p],
            device_id={"grow": lax.rem(me + n - 1, n)}, device_id_type=MESH)
        for p, (r, c) in enumerate([(0, 1), (0, 2), (1, 1), (1, 2)])
    ]

    @pl.when(has_next)
    def _():
        for copy in to_next:
            copy.start()

    @pl.when(has_prev)
    def _():
        for copy in to_prev:
            copy.start()

    @pl.when(jnp.logical_not(has_prev))
    def _():
        before[...] = jnp.zeros_like(before)

    @pl.when(jnp.logical_not(has_next))
    def _():
        after[...] = jnp.zeros_like(after)

    def arrive(p):
        @pl.when(has_prev)
        def _():
            to_next[p].wait_recv()

        @pl.when(has_next)
        def _():
            to_prev[p].wait_recv()

    def on_diagonal():
        return lax.broadcasted_iota(jnp.int32, (edge, edge), 0) == lax.broadcasted_iota(
            jnp.int32, (edge, edge), 1)

    def mask(e, c):
        row = jnp.clip(me * rows + e - 2, 0, row_total - 1)
        return pattern[c, row].astype(F32)

    def lanes(c):
        return slice(c * edge, (c + 1) * edge)

    def put_a(e, c, block):
        value = -block
        if c == 1:
            value = jnp.where(on_diagonal(), potential[0] + value, value)
        store(a, (e, slice(None), lanes(c)), value * mask(e, c))

    left_of = {0: slice(0, 2 * edge), 1: slice(0, 3 * edge), 2: slice(edge, 3 * edge)}
    right_of = {0: slice(edge, 3 * edge), 1: slice(0, 3 * edge), 2: slice(0, 2 * edge)}
    full = slice(None)

    def filtered(left, right, e, c, transposed=False):
        right_at = (e + c - 1, full, right_of[c]) if transposed else (e + c - 1, right_of[c], full)
        return product(left, right, (e, full, left_of[c]), right_at, transposed)

    def shifted(square, e, c):
        value = -square
        if c == 1:
            value = jnp.where(on_diagonal(), 3.0 + value, value)
        return value * mask(e, c)

    def column_at(e, c):
        return (e + c - 1, lanes(2 - c), full)

    def diagonal(e):
        high, low = ah[e], al[e]
        dims = (((1,), (1,)), ((), ()))
        cross = lax.dot_general(high, low, dims, preferred_element_type=F32)
        square = lax.dot_general(high, high, dims, preferred_element_type=F32)
        store(s, column_at(e, 1), shifted((cross + cross.T) + square, e, 1))

    def upper(e):
        value = shifted(filtered(a, a, e, 2, True), e, 2)
        store(s, column_at(e, 2), value)
        store(s, column_at(e + 1, 0), value.T)

    def f2(e, slots=(0, 1, 2)):
        for c in slots:
            value = filtered(a, s, e, c) * (0.5 * mask(e, c))
            store(cr, (e, full, lanes(c)), value)
            store(cc, column_at(e, c), value)

    def f3(e, slots=(0, 1, 2)):
        for c in slots:
            store(s2, column_at(e, c), shifted(filtered(cr, cc, e, c), e, c))

    def f4(e, slots=(0, 1, 2)):
        for c in slots:
            value = filtered(cr, s2, e, c) * (0.5 * mask(e, c))
            out[e - 2, c] = value
            if c == 1:
                trace_tile[...] += jnp.sum(jnp.where(on_diagonal(), value, 0.0), axis=0, keepdims=True)

    def span(function, low, high):
        pl.loop(low, high)(function)

    def both(function, low, high):
        @pl.loop(0, 2)
        def _(k):
            function(low + k * (high - low))

    trace_tile[...] = jnp.zeros_like(trace_tile)
    lo, hi = 2, rows + 1
    for r in range(rows):
        loads[r].wait()
        for c in range(3):
            put_a(r + 2, c, stage[r, c])
    span(diagonal, lo, hi + 1)
    span(upper, lo, hi)
    span(f2, lo + 1, hi)
    span(f3, lo + 2, hi - 1)

    put_a(lo - 1, 2, stage[0, 0].T)
    put_a(hi + 1, 0, stage[last, 2].T)
    arrive(0)
    put_a(lo - 1, 1, before[0])
    put_a(hi + 1, 1, after[0])
    both(upper, lo - 1, hi)
    f2(lo, (1, 2))
    f2(hi, (0, 1))
    f2(lo - 1, (2,))
    f2(hi + 1, (0,))
    both(f3, lo + 1, hi - 1)
    span(f4, lo + 2, hi - 1)

    arrive(1)
    put_a(lo - 1, 0, before[1])
    put_a(lo - 2, 2, before[1].T)
    put_a(hi + 1, 2, after[1])
    put_a(hi + 2, 0, after[1].T)
    both(diagonal, lo - 1, hi + 1)
    f2(lo, (0,))
    f2(hi, (2,))
    f3(lo, (1, 2))
    f3(hi, (0, 1))
    both(f4, lo + 1, hi - 1)

    arrive(2)
    put_a(lo - 2, 1, before[2])
    put_a(hi + 2, 1, after[2])
    both(upper, lo - 2, hi + 1)
    f2(lo - 1, (1,))
    f2(hi + 1, (1,))
    f3(lo, (0,))
    f3(hi, (2,))
    f3(lo - 1, (2,))
    f3(hi + 1, (0,))
    f4(lo, (1, 2))
    f4(hi, (0, 1))

    parts[me] = jnp.broadcast_to(trace_tile[...], parts.shape[1:])

    def part_copy(target, slot):
        return pltpu.make_async_remote_copy(
            src_ref=parts.at[me], dst_ref=parts.at[me], send_sem=part_send.at[target],
            recv_sem=part_recv.at[slot], device_id={"grow": target}, device_id_type=MESH)

    @pl.loop(1, n)
    def _(k):
        part_copy(lax.rem(me + k, n), me).start()

    arrive(3)
    put_a(lo - 2, 0, before[3])
    put_a(hi + 2, 2, after[3])
    both(diagonal, lo - 2, hi + 2)
    f2(lo - 1, (0,))
    f2(hi + 1, (2,))
    f2(lo - 2, (2,))
    f2(hi + 2, (0,))
    f3(lo - 1, (1,))
    f3(hi + 1, (1,))
    f4(lo, (0,))
    f4(hi, (2,))

    @pl.when(has_next)
    def _():
        for copy in to_next:
            copy.wait_send()

    @pl.when(has_prev)
    def _():
        for copy in to_prev:
            copy.wait_send()

    @pl.loop(1, n)
    def _(k):
        other = lax.rem(me + k, n)
        copy = part_copy(other, other)
        copy.wait_recv()
        copy.wait_send()

    order = float(row_total * edge)
    total = jnp.sum(jnp.sum(parts[...], axis=0)[0:1])
    occupation[0] = (order + total) / (2.0 * order)


def local(n, hamiltonian, pattern, potential):
    rows, edge = hamiltonian.shape[0], hamiltonian.shape[2]
    wide, tall = (rows + 4, edge, 3 * edge), (rows + 4, 3 * edge, edge)
    pairs = [wide, tall, wide, tall, tall]
    any_space = pl.BlockSpec(memory_space=pl.ANY)
    scalars = pl.BlockSpec(memory_space=pltpu.SMEM)
    sems = pltpu.SemaphoreType.DMA
    return pl.pallas_call(
        functools.partial(kernel, n),
        out_shape=(pltpu.VMEM(hamiltonian.shape, F32), jax.ShapeDtypeStruct((1,), F32)),
        in_specs=[any_space, scalars, scalars],
        out_specs=(pl.BlockSpec(memory_space=pltpu.VMEM), scalars),
        scratch_shapes=[
            pltpu.VMEM((rows, 3, edge, edge), F32),
            pltpu.VMEM((PIECES, edge, edge), F32),
            pltpu.VMEM((PIECES, edge, edge), F32),
            pltpu.VMEM((n, 8, edge), F32),
            pltpu.VMEM((1, edge), F32),
            *[pltpu.VMEM(shape, BF16) for shape in pairs for _ in range(2)],
            sems((rows,)), sems((PIECES,)), sems((PIECES,)), sems((PIECES,)), sems((PIECES,)),
            sems((n,)), sems((n,)),
        ],
        compiler_params=pltpu.CompilerParams(
            collective_id=0, has_side_effects=True, vmem_limit_bytes=VMEM_LIMIT),
        name="sign_iterations",
    )(hamiltonian, pattern.T, potential)


def solution(mesh):
    in_specs = (P(("reps", "grow"), None, None, None), P(), P("reps"))
    out_specs = (P(("reps", "grow"), None, None, None), P("reps"))
    return jax.shard_map(
        functools.partial(local, mesh.shape["grow"]),
        mesh=mesh, in_specs=in_specs, out_specs=out_specs, check_vma=False)
```
